32 devices in a mesh: groups: 2 (over y), context: 8 (over z, x), tensor: 2 (over core).
Axes of the slice: x: 2, y: 2, z: 4, core: 2. Of those that a mesh axis runs over, the one named last changes fastest.
Arguments:
- self_queries: bfloat16 [1280, 2048], P(('groups', 'context'), 'tensor'), parts along dimension 0, may hold values from -512 to 512
- self_keys: bfloat16 [1280, 512], P(('groups', 'context'), 'tensor'), parts along dimension 0, may hold values from -6 to 6
- self_values: bfloat16 [1280, 512], P(('groups', 'context'), 'tensor'), parts along dimension 0, may hold values from -6 to 6
- cross_queries: bfloat16 [1280, 2048], P(('groups', 'context'), 'tensor'), parts along dimension 0, may hold values from -512 to 512
- cross_keys: bfloat16 [384, 512], P(('groups', 'context'), 'tensor'), parts along dimension 0, may hold values from -6 to 6
- cross_values: bfloat16 [384, 512], P(('groups', 'context'), 'tensor'), parts along dimension 0, may hold values from -6 to 6
- span_order: int32 [32], P('groups'), parts along dimension 0, may hold values from 0 to 15, as said below
Outputs:
- self_out: bfloat16 [1280, 2048], P(('groups', 'context'), 'tensor'), parts along dimension 0
- cross_out: bfloat16 [1280, 2048], P(('groups', 'context'), 'tensor'), parts along dimension 0
The draws below stay inside these ranges and needn't reach their ends.
There are 2 independent parts, one for each index of `groups`. The reference program is written for one: setup_inputs(seed, part) draws one part's arguments, and reference() takes and returns one part's arrays. A program takes and returns all parts, laid end to end along the dimension named above; each array names one. Nothing has to cross between parts.
Inputs may be any that keep to these rules, and one draw needn't show every extreme that they name: `span_order`: each of 0 to 15 appears once, and entries 2 d and 2 d + 1 sum to 15.
All inputs are finite; a program needn't handle non-finite values.
Results may differ from the reference program's by a relative error of at most 0.012.
The reference program's roundings to bfloat16 on the way count: a program that leaves them out, or rounds other values in their place, can miss the bound.
Values may be sent and summed in bfloat16 or wider, within the bound.
A program may use at most 128 MiB of HBM per device.

```python
import jax
import jax.numpy as jnp
from jax import lax

HEAD_DIM = 128
HEADS = 16
KV_HEADS = 4
TEXT = 640
IMAGE = 192
SPAN = 40
SPANS = 16


def self_draw(key):
    key_query, key_key = jax.random.split(jax.random.fold_in(key, 17), 2)
    key_rows = jnp.clip(jax.random.normal(key_key, (TEXT, KV_HEADS, HEAD_DIM), jnp.float32), -6.0, 6.0)
    query_rows = jnp.clip(2.5 * jax.random.normal(key_query, (TEXT, HEADS, HEAD_DIM), jnp.float32), -15.0, 15.0)
    return (query_rows.reshape(TEXT, HEADS * HEAD_DIM), key_rows.reshape(TEXT, KV_HEADS * HEAD_DIM))


def cross_draw(key):
    key_query, key_key = jax.random.split(jax.random.fold_in(key, 29), 2)
    key_rows = jnp.clip(jax.random.normal(key_key, (IMAGE, KV_HEADS, HEAD_DIM), jnp.float32), -6.0, 6.0)
    query_rows = jnp.clip(2.5 * jax.random.normal(key_query, (TEXT, HEADS, HEAD_DIM), jnp.float32), -15.0, 15.0)
    return (query_rows.reshape(TEXT, HEADS * HEAD_DIM), key_rows.reshape(IMAGE, KV_HEADS * HEAD_DIM))


def draw_self_queries(key, part):
    return self_draw(key)[0].astype(jnp.bfloat16)


def draw_self_keys(key, part):
    return self_draw(key)[1].astype(jnp.bfloat16)


def draw_cross_queries(key, part):
    return cross_draw(key)[0].astype(jnp.bfloat16)


def draw_cross_keys(key, part):
    return cross_draw(key)[1].astype(jnp.bfloat16)


def draw_span_order(key, part):
    half_count = SPANS // 2
    key_owner, key_flip = jax.random.split(jax.random.fold_in(key, 5))
    owner = jax.random.permutation(key_owner, half_count).astype(jnp.int32)
    flipped = jax.random.randint(key_flip, (half_count,), 0, 2)
    late_span = SPANS - 1 - owner
    first_span = jnp.where(flipped == 1, late_span, owner)
    second_span = jnp.where(flipped == 1, owner, late_span)
    return jnp.stack([first_span, second_span], 1).reshape(-1).astype(jnp.int32)


def block_levels(own_key, dims, cuts, low, top_value):
    level = 1.0
    for position, shards_of in cuts:
        heights = jax.random.uniform(jax.random.fold_in(jax.random.fold_in(own_key, 6), position), (shards_of,), jnp.float32, low / len(cuts), top_value / len(cuts))
        level = level * jnp.repeat(jnp.exp(heights), dims[position] // shards_of).reshape((-1,) + (1,) * (len(dims) - 1 - position))
    return level


def noise(key, dims, scale, most, cuts=(), kind=jnp.bfloat16):
    array = scale * jax.random.normal(key, dims, jnp.float32)
    if cuts:
        array = array * block_levels(key, dims, cuts, -0.22, 0.18)
    return jnp.clip(array, -most, most).astype(kind)


def setup_inputs(seed: int = 0, part: int = 0) -> dict:
    arg_keys = jax.random.split(jax.random.key(seed), 8)
    own_keys = jax.random.split(jax.random.fold_in(arg_keys[7], part), 8)
    self_queries = draw_self_queries(jax.random.fold_in(jax.random.fold_in(arg_keys[7], part), 71), part)
    self_keys = draw_self_keys(jax.random.fold_in(jax.random.fold_in(arg_keys[7], part), 71), part)
    self_values = noise(own_keys[2], (TEXT, KV_HEADS * HEAD_DIM), 1.0, 6.0, ((0, 8), (1, 2)))
    cross_queries = draw_cross_queries(jax.random.fold_in(jax.random.fold_in(arg_keys[7], part), 71), part)
    cross_keys = draw_cross_keys(jax.random.fold_in(jax.random.fold_in(arg_keys[7], part), 71), part)
    cross_values = noise(own_keys[5], (IMAGE, KV_HEADS * HEAD_DIM), 1.0, 6.0, ((0, 8), (1, 2)))
    span_order = draw_span_order(jax.random.fold_in(jax.random.fold_in(arg_keys[7], part), 71), part)
    return {"self_queries": self_queries, "self_keys": self_keys, "self_values": self_values, "cross_queries": cross_queries, "cross_keys": cross_keys, "cross_values": cross_values, "span_order": span_order}


def rotary(values, places):
    half_dim = values.shape[-1] // 2
    frequency = 500000.0 ** (-(jnp.arange(half_dim, dtype=jnp.float32) * 2.0) / values.shape[-1])
    angles = places.astype(jnp.float32)[:, None] * frequency[None, :]
    cosine = jnp.cos(angles)[:, None, :]
    sine_part = jnp.sin(angles)[:, None, :]
    first_half = values[..., :half_dim]
    second_half = values[..., half_dim:]
    return jnp.concatenate([first_half * cosine - second_half * sine_part, second_half * cosine + first_half * sine_part], -1)


def attend_block(queries, key_rows, value_rows, query_places, key_places):
    scores = jnp.einsum("qkgd,rkd->kgqr", queries.astype(jnp.float32), key_rows.astype(jnp.float32)) * (HEAD_DIM ** -0.5)
    if key_places is not None:
        allowed = key_places[None, :] <= query_places[:, None]
        scores = jnp.where(allowed[None, None], scores, -jnp.inf)
    row_peak = jnp.max(scores, -1, keepdims=True)
    weights = jnp.exp(scores - row_peak)
    weight_sum = jnp.sum(weights, -1)
    rounded = lax.optimization_barrier(weights.astype(jnp.bfloat16))
    mixed_sum = jnp.einsum("kgqr,rkd->qkgd", rounded.astype(jnp.float32), value_rows.astype(jnp.float32))
    return mixed_sum / jnp.transpose(weight_sum, (2, 0, 1))[..., None]


def attention(queries, key_rows, value_rows, query_places, key_places):
    row_total = queries.shape[0]
    block_rows = min(512, row_total)
    while row_total % block_rows != 0:
        block_rows = block_rows // 2
    query_blocks = queries.reshape((row_total // block_rows, block_rows) + queries.shape[1:])
    if key_places is None:
        def per_block(query_block):
            return attend_block(query_block, key_rows, value_rows, None, None)
        result = lax.map(per_block, query_blocks)
    else:
        place_blocks = query_places.reshape(row_total // block_rows, block_rows)

        def per_masked(arrived):
            return attend_block(arrived[0], key_rows, value_rows, arrived[1], key_places)
        result = lax.map(per_masked, (query_blocks, place_blocks))
    return result.reshape(row_total, -1).astype(jnp.bfloat16)


def reference(self_queries, self_keys, self_values, cross_queries, cross_keys, cross_values, span_order):
    group_size = HEADS // KV_HEADS
    places = (span_order[:, None] * SPAN + jnp.arange(SPAN, dtype=jnp.int32)[None, :]).reshape(-1).astype(jnp.int32)
    text_queries = rotary(self_queries.astype(jnp.float32).reshape(TEXT, HEADS, HEAD_DIM), places).astype(jnp.bfloat16)
    text_queries = lax.optimization_barrier(text_queries).reshape(TEXT, KV_HEADS, group_size, HEAD_DIM)
    text_keys = rotary(self_keys.astype(jnp.float32).reshape(TEXT, KV_HEADS, HEAD_DIM), places).astype(jnp.bfloat16)
    text_keys = lax.optimization_barrier(text_keys)
    self_out = attention(text_queries, text_keys, self_values.reshape(TEXT, KV_HEADS, HEAD_DIM), places, places)
    image_queries = cross_queries.reshape(TEXT, KV_HEADS, group_size, HEAD_DIM)
    cross_out = attention(image_queries, cross_keys.reshape(IMAGE, KV_HEADS, HEAD_DIM), cross_values.reshape(IMAGE, KV_HEADS, HEAD_DIM), None, None)
    return (self_out, cross_out)
```

```python
import functools
import math

import jax
import jax.numpy as jnp
import numpy as np
from jax import lax
from jax.experimental import pallas as pl
from jax.experimental.pallas import tpu as pltpu
from jax.sharding import PartitionSpec as P

HEAD_DIM = 128
HEADS = 16
KV_HEADS = 4
GROUP = HEADS // KV_HEADS
NEG_FILL = -1e30
SCALE = HEAD_DIM ** (-0.5) * math.log2(math.e)
UP, DOWN, RIGHT, LEFT = range(4)


def rotary_tables(spans, span_len):
    half = HEAD_DIM // 2
    frequency = 500000.0 ** (-(np.arange(half) * 2.0) / HEAD_DIM)
    frequency = np.concatenate([frequency, frequency])
    base = (np.arange(spans) * span_len)[:, None] * frequency[None, :]
    inner = np.arange(span_len)[:, None] * frequency[None, :]
    sign = np.where(np.arange(HEAD_DIM) < half, -1.0, 1.0)[None, :]
    bases = np.stack([np.cos(base), np.sin(base)])
    inners = np.stack([np.cos(inner), np.sin(inner), np.cos(inner) * sign, np.sin(inner) * sign])
    return bases.astype(np.float32), inners.astype(np.float32)


def for_range(low, high, step):
    if high - low <= 4:
        for index in range(low, high):
            step(index)
    else:
        lax.fori_loop(low, high, lambda index, unused: (step(index), 0)[1], 0)


def is_zero(distance):
    return isinstance(distance, int) and distance == 0


def kernel(
    n, nx,
    order, q_hbm, k_hbm, v_hbm, cq_hbm, ck_hbm, cv_hbm, bases_hbm, inners_hbm,
    out_hbm, cout_hbm,
    text, image, q_in, cq_in, bases, inners, q_rot, peak, total, mixed, out_v, cout_v,
    load_sem, out_sem, text_send, text_recv, image_send, image_recv,
):
    nz = n // nx
    me = lax.axis_index("context")
    z, x = me // nx, lax.rem(me, nx)
    rows = q_in.shape[0]
    span_len = rows // 2
    kv_local = text.shape[3] // HEAD_DIM
    image_rows = image.shape[2]

    exists = (z < nz - 1, z > 0, x < nx - 1, x > 0)
    neighbour = (me + nx, me - nx, me + 1, me - 1)

    kv_loads = [
        pltpu.make_async_copy(k_hbm, text.at[me, 0], load_sem.at[0]),
        pltpu.make_async_copy(v_hbm, text.at[me, 1], load_sem.at[1]),
        pltpu.make_async_copy(ck_hbm, image.at[me, 0], load_sem.at[2]),
        pltpu.make_async_copy(cv_hbm, image.at[me, 1], load_sem.at[3]),
    ]
    other_loads = [
        pltpu.make_async_copy(bases_hbm, bases, load_sem.at[4]),
        pltpu.make_async_copy(inners_hbm, inners, load_sem.at[5]),
        pltpu.make_async_copy(q_hbm, q_in, load_sem.at[6]),
        pltpu.make_async_copy(cq_hbm, cq_in, load_sem.at[7]),
    ]
    for load in kv_loads + other_loads:
        load.start()

    barrier = pltpu.get_barrier_semaphore()
    for way in range(4):
        @pl.when(exists[way])
        def _():
            pl.semaphore_signal(
                barrier, inc=1, device_id={"context": neighbour[way]},
                device_id_type=pl.DeviceIdType.MESH,
            )
    pl.semaphore_wait(barrier, sum(e.astype(jnp.int32) for e in exists))
    for load in kv_loads:
        load.wait()

    def text_copy(slot, part, way):
        return pltpu.make_async_remote_copy(
            src_ref=text.at[slot, part], dst_ref=text.at[slot, part],
            send_sem=text_send.at[slot, part, way], recv_sem=text_recv.at[slot, part],
            device_id={"context": neighbour[way]}, device_id_type=pl.DeviceIdType.MESH,
        )

    def image_copy(slot, way):
        return pltpu.make_async_remote_copy(
            src_ref=image.at[slot], dst_ref=image.at[slot],
            send_sem=image_send.at[slot, way], recv_sem=image_recv.at[slot],
            device_id={"context": neighbour[way]}, device_id_type=pl.DeviceIdType.MESH,
        )

    def ways_of(rel_first, rel_second, first, second):
        ways = []
        if rel_second == 0:
            if rel_first <= 0:
                ways.append(first[0])
            if rel_first >= 0:
                ways.append(first[1])
            ways += list(second)
        else:
            ways.append(second[0] if rel_second < 0 else second[1])
        return ways

    def place(rel, distance, own, count):
        at = own + rel * distance
        valid = True if rel == 0 else (at >= 0 if rel < 0 else at < count)
        return at, valid

    def visit(rel_z, dz, rel_x, dx, action):
        at_z, valid_z = place(rel_z, dz, z, nz)
        at_x, valid_x = place(rel_x, dx, x, nx)
        slot = at_z * nx + at_x
        if rel_z == 0 and rel_x == 0:
            action(slot)
            return
        valid = valid_z if rel_x == 0 else (valid_x if rel_z == 0 else jnp.logical_and(valid_z, valid_x))
        pl.when(valid)(lambda: action(slot))

    def send_text(slot, part, rel_z, rel_x, op):
        for way in ways_of(rel_z, rel_x, (UP, DOWN), (RIGHT, LEFT)):
            pl.when(exists[way])(lambda way=way: getattr(text_copy(slot, part, way), op)())

    def send_image(slot, rel_z, rel_x, op):
        for way in ways_of(rel_x, rel_z, (RIGHT, LEFT), (UP, DOWN)):
            pl.when(exists[way])(lambda way=way: getattr(image_copy(slot, way), op)())

    def relay_text(rel_z, dz, rel_x, dx):
        def action(slot):
            for part in range(2):
                text_copy(slot, part, UP).wait_recv()
                send_text(slot, part, rel_z, rel_x, "start")
        visit(rel_z, dz, rel_x, dx, action)

    def relay_image(rel_z, dz, rel_x, dx):
        def action(slot):
            image_copy(slot, UP).wait_recv()
            send_image(slot, rel_z, rel_x, "start")
        visit(rel_z, dz, rel_x, dx, action)

    send_text(me, 0, 0, 0, "start")
    send_text(me, 1, 0, 0, "start")
    send_image(me, 0, 0, "start")

    for load in other_loads:
        load.wait()

    def angles(slot):
        cosines, sines, starts = [], [], []
        for part in range(2):
            span = order[2 * slot + part]
            base_cos = bases[0, pl.ds(span, 1), :]
            base_sin = bases[1, pl.ds(span, 1), :]
            cosines.append(base_cos * inners[0] - base_sin * inners[1])
            sines.append(base_sin * inners[2] + base_cos * inners[3])
            starts.append(span * span_len)
        return jnp.concatenate(cosines, 0), jnp.concatenate(sines, 0), starts

    def rotate(values, cosine, sine):
        values = values.astype(jnp.float32)
        turned = pltpu.roll(values, HEAD_DIM // 2, 1)
        return (values * cosine + turned * sine).astype(jnp.bfloat16)

    def positions(starts, shape, axis):
        index = lax.broadcasted_iota(jnp.int32, shape, axis)
        return jnp.where(index < span_len, starts[0] + index, starts[1] + index - span_len)

    own_cos, own_sin, own_starts = angles(me)
    for head in range(kv_local * GROUP):
        q_rot[head // GROUP, pl.ds(head % GROUP * rows, rows), :] = rotate(
            q_in[:, head * HEAD_DIM:(head + 1) * HEAD_DIM], own_cos, own_sin)

    def dot_nt(a, b):
        return lax.dot_general(a, b, (((1,), (1,)), ((), ())), preferred_element_type=jnp.float32)

    def block(slot, first):
        cosine, sine, starts = angles(slot)
        allowed = positions(starts, (rows, rows), 1) <= positions(own_starts, (rows, rows), 0)
        for head in range(kv_local):
            columns = slice(head * HEAD_DIM, (head + 1) * HEAD_DIM)
            keys = rotate(text[slot, 0, :, columns], cosine, sine)
            scores = dot_nt(q_rot[head], keys) * SCALE
            scores = jnp.where(allowed[None], scores.reshape(GROUP, rows, rows), NEG_FILL)
            scores = scores.reshape(GROUP * rows, rows)
            top = jnp.max(scores, -1, keepdims=True)
            if not first:
                old = peak[head]
                top = jnp.maximum(top, old)
            weights = jnp.exp2(scores - top)
            summed = jnp.sum(weights, -1, keepdims=True)
            product = jnp.dot(
                weights.astype(jnp.bfloat16), text[slot, 1, :, columns],
                preferred_element_type=jnp.float32)
            if not first:
                factor = jnp.exp2(old - top)
                summed = summed + total[head] * factor
                product = product + mixed[head] * factor
            peak[head] = top
            total[head] = summed
            mixed[head] = product

    def blocks_at(dz, columns_of):
        count_x, at_x = columns_of
        low = (z - dz >= 0).astype(jnp.int32)
        high = (z + dz < nz).astype(jnp.int32)
        count = low + high if not is_zero(dz) else 1

        def step(index, unused):
            side, column = index // count_x, lax.rem(index, count_x)
            at_z = jnp.where(jnp.logical_and(side == 0, low == 1), z - dz, z + dz)
            block(at_z * nx + at_x(column), False)
            return 0

        lax.fori_loop(0, count * count_x, step, 0)

    own_column = (1, lambda column: x)
    other_columns = (nx - 1, lambda column: lax.rem(x + 1 + column, nx))

    block(me, True)

    sides = (-1, 1)

    def across_image(rel_z, dz):
        if rel_z != 0:
            relay_image(rel_z, dz, 0, 0)
        for rel_x in sides:
            for_range(1, nx, lambda dx: relay_image(rel_z, dz, rel_x, dx))

    def across_text(dz):
        for rel_z in ((0,) if is_zero(dz) else sides):
            for rel_x in sides:
                for_range(1, nx, lambda dx: relay_text(rel_z, dz, rel_x, dx))

    across_image(0, 0)

    def stage(dz, before):
        for rel_z in sides:
            relay_text(rel_z, dz, 0, 0)
        for rel_z in sides:
            across_image(rel_z, dz)
        if nx > 1:
            across_text(before)
            blocks_at(before, other_columns)
        blocks_at(dz, own_column)

    if nz > 1:
        stage(1, 0)
        for_range(2, nz, lambda dz: stage(dz, dz - 1))

    keys_all = image[:, 0].astype(jnp.float32).reshape(n * image_rows, -1).astype(jnp.bfloat16)
    values_all = image[:, 1].astype(jnp.float32).reshape(n * image_rows, -1).astype(jnp.bfloat16)
    for head in range(kv_local):
        columns = slice(head * HEAD_DIM, (head + 1) * HEAD_DIM)
        first_head = head * GROUP
        queries = jnp.concatenate(
            [cq_in[:, (first_head + g) * HEAD_DIM:(first_head + g + 1) * HEAD_DIM] for g in range(GROUP)], 0)
        scores = dot_nt(queries, keys_all[:, columns]) * SCALE
        weights = jnp.exp2(scores - jnp.max(scores, -1, keepdims=True))
        summed = jnp.sum(weights, -1, keepdims=True)
        product = jnp.dot(
            weights.astype(jnp.bfloat16), values_all[:, columns], preferred_element_type=jnp.float32)
        result = (product / summed).astype(jnp.bfloat16)
        for g in range(GROUP):
            cout_v[:, (first_head + g) * HEAD_DIM:(first_head + g + 1) * HEAD_DIM] = result[g * rows:(g + 1) * rows]
    cross_store = pltpu.make_async_copy(cout_v, cout_hbm, out_sem.at[0])
    cross_store.start()

    if nx > 1:
        last = nz - 1
        across_text(last)
        blocks_at(last, other_columns)

    for head in range(kv_local):
        result = (mixed[head] / total[head]).astype(jnp.bfloat16)
        for g in range(GROUP):
            at = head * GROUP + g
            out_v[:, at * HEAD_DIM:(at + 1) * HEAD_DIM] = result[g * rows:(g + 1) * rows]
    self_store = pltpu.make_async_copy(out_v, out_hbm, out_sem.at[1])
    self_store.start()

    def drain(rel_z, dz, rel_x, dx):
        def action(slot):
            for part in range(2):
                send_text(slot, part, rel_z, rel_x, "wait_send")
            send_image(slot, rel_z, rel_x, "wait_send")
        visit(rel_z, dz, rel_x, dx, action)

    def drain_row(rel_z, dz):
        drain(rel_z, dz, 0, 0)
        for rel_x in sides:
            for_range(1, nx, lambda dx: drain(rel_z, dz, rel_x, dx))

    drain_row(0, 0)
    for rel_z in sides:
        for_range(1, nz, lambda dz: drain_row(rel_z, dz))
    cross_store.wait()
    self_store.wait()


def body(n, nx, self_queries, self_keys, self_values, cross_queries, cross_keys, cross_values, span_order):
    rows, width = self_queries.shape
    kv_width = self_keys.shape[1]
    kv_local = kv_width // HEAD_DIM
    image_rows = cross_keys.shape[0]
    bases, inners = rotary_tables(span_order.shape[0], rows // 2)
    anywhere = pl.BlockSpec(memory_space=pl.ANY)
    result = jax.ShapeDtypeStruct((rows, width), jnp.bfloat16)
    return pl.pallas_call(
        functools.partial(kernel, n, nx),
        out_shape=(result, result),
        in_specs=[pl.BlockSpec(memory_space=pltpu.SMEM)] + [anywhere] * 8,
        out_specs=(anywhere, anywhere),
        scratch_shapes=[
            pltpu.VMEM((n, 2, rows, kv_width), jnp.bfloat16),
            pltpu.VMEM((n, 2, image_rows, kv_width), jnp.bfloat16),
            pltpu.VMEM((rows, width), jnp.bfloat16),
            pltpu.VMEM((rows, width), jnp.bfloat16),
            pltpu.VMEM(bases.shape, jnp.float32),
            pltpu.VMEM(inners.shape, jnp.float32),
            pltpu.VMEM((kv_local, GROUP * rows, HEAD_DIM), jnp.bfloat16),
            pltpu.VMEM((kv_local, GROUP * rows, 1), jnp.float32),
            pltpu.VMEM((kv_local, GROUP * rows, 1), jnp.float32),
            pltpu.VMEM((kv_local, GROUP * rows, HEAD_DIM), jnp.float32),
            pltpu.VMEM((rows, width), jnp.bfloat16),
            pltpu.VMEM((rows, width), jnp.bfloat16),
            pltpu.SemaphoreType.DMA((8,)),
            pltpu.SemaphoreType.DMA((2,)),
            pltpu.SemaphoreType.DMA((n, 2, 4)),
            pltpu.SemaphoreType.DMA((n, 2)),
            pltpu.SemaphoreType.DMA((n, 4)),
            pltpu.SemaphoreType.DMA((n,)),
        ],
        compiler_params=pltpu.CompilerParams(collective_id=0, has_side_effects=True),
    )(span_order, self_queries, self_keys, self_values, cross_queries, cross_keys, cross_values, bases, inners)


def fast_axis(mesh, n):
    line = mesh.devices[0, :, 0]
    coords = [getattr(device, "coords", None) for device in line]
    if any(c is None for c in coords):
        return 1
    nx = len({c[0] for c in coords})
    return nx if n % nx == 0 else 1


def solution(mesh):
    n = mesh.shape["context"]
    both = P(("groups", "context"), "tensor")
    return jax.shard_map(
        functools.partial(body, n, fast_axis(mesh, n)), mesh=mesh,
        in_specs=(both,) * 6 + (P("groups"),), out_specs=(both, both), check_vma=False)
```

```python
import functools
import math

import jax
import jax.numpy as jnp
import numpy as np
from jax import lax
from jax.experimental import pallas as pl
from jax.experimental.pallas import tpu as pltpu
from jax.sharding import PartitionSpec as P

HEAD_DIM = 128
HEADS = 16
KV_HEADS = 4
GROUP = HEADS // KV_HEADS
NEG_FILL = -1e30
SCALE = HEAD_DIM ** (-0.5) * math.log2(math.e)


def rotary_tables(spans, span_len):
    half = HEAD_DIM // 2
    frequency = 500000.0 ** (-(np.arange(half) * 2.0) / HEAD_DIM)
    frequency = np.concatenate([frequency, frequency])
    base = (np.arange(spans) * span_len)[:, None] * frequency[None, :]
    inner = np.arange(span_len)[:, None] * frequency[None, :]
    sign = np.where(np.arange(HEAD_DIM) < half, -1.0, 1.0)[None, :]
    bases = np.stack([np.cos(base), np.sin(base)])
    inners = np.stack([np.cos(inner), np.sin(inner), np.cos(inner) * sign, np.sin(inner) * sign])
    return bases.astype(np.float32), inners.astype(np.float32)


def doubling(order):
    held, steps = [0], []
    for mask in order:
        steps.append((mask, list(held)))
        held += [item ^ mask for item in held]
    return steps


def kernel(
    n, nx,
    order, q_hbm, k_hbm, v_hbm, cq_hbm, ck_hbm, cv_hbm, bases_hbm, inners_hbm,
    out_v, cout_v,
    text, image, q_in, cq_in, bases, inners, q_rot, peak, total, mixed,
    load_sem, text_send, text_recv, image_send, image_recv,
):
    me = lax.axis_index("context")
    rows = q_in.shape[0]
    span_len = rows // 2
    kv_local = text.shape[3] // HEAD_DIM
    image_rows = image.shape[2]

    x_masks = [1 << b for b in reversed(range(nx.bit_length() - 1))]
    z_masks = [nx << b for b in reversed(range((n // nx).bit_length() - 1))]
    masks = z_masks + x_masks
    text_steps = doubling(z_masks + x_masks)
    image_steps = doubling(z_masks[:1] + x_masks + z_masks[1:])

    def flipped(index, item):
        for mask in masks:
            bit = (item // mask) % 2
            index = index + mask * bit * (1 - 2 * ((index // mask) % 2))
        return index

    partner = {mask: flipped(me, mask) for mask in masks}

    kv_loads = [
        pltpu.make_async_copy(k_hbm, text.at[0, 0], load_sem.at[0]),
        pltpu.make_async_copy(v_hbm, text.at[0, 1], load_sem.at[1]),
        pltpu.make_async_copy(ck_hbm, image.at[0, 0], load_sem.at[2]),
        pltpu.make_async_copy(cv_hbm, image.at[0, 1], load_sem.at[3]),
    ]
    other_loads = [
        pltpu.make_async_copy(bases_hbm, bases, load_sem.at[4]),
        pltpu.make_async_copy(inners_hbm, inners, load_sem.at[5]),
        pltpu.make_async_copy(q_hbm, q_in, load_sem.at[6]),
        pltpu.make_async_copy(cq_hbm, cq_in, load_sem.at[7]),
    ]
    for load in kv_loads:
        load.start()
    barrier = pltpu.get_barrier_semaphore()
    for mask in masks:
        pl.semaphore_signal(
            barrier, inc=1, device_id={"context": partner[mask]},
            device_id_type=pl.DeviceIdType.MESH)
    for load in other_loads:
        load.start()
    for load in kv_loads:
        load.wait()
    pl.semaphore_wait(barrier, len(masks))

    started = []

    def text_copy(item, part, mask):
        way = masks.index(mask)
        return pltpu.make_async_remote_copy(
            src_ref=text.at[item, part], dst_ref=text.at[item ^ mask, part],
            send_sem=text_send.at[item, part, way], recv_sem=text_recv.at[item ^ mask, part],
            device_id={"context": partner[mask]}, device_id_type=pl.DeviceIdType.MESH)

    def image_copy(item, mask):
        way = masks.index(mask)
        return pltpu.make_async_remote_copy(
            src_ref=image.at[item], dst_ref=image.at[item ^ mask],
            send_sem=image_send.at[item, way], recv_sem=image_recv.at[item ^ mask],
            device_id={"context": partner[mask]}, device_id_type=pl.DeviceIdType.MESH)

    def start(copy):
        copy.start()
        started.append(copy)

    def forward_text(item, part):
        for mask, held in text_steps:
            if item in held:
                start(text_copy(item, part, mask))

    def forward_image(item):
        for mask, held in image_steps:
            if item in held:
                start(image_copy(item, mask))

    def arrive_text(item):
        for part in range(2):
            text_copy(item ^ masks[0], part, masks[0]).wait_recv()
            forward_text(item, part)

    def arrive_image(item):
        image_copy(item ^ masks[0], masks[0]).wait_recv()
        forward_image(item)

    forward_text(0, 0)
    forward_text(0, 1)
    forward_image(0)

    for load in other_loads:
        load.wait()

    def angles(place):
        cosines, sines, starts = [], [], []
        for part in range(2):
            span = order[2 * place + part]
            base_cos = bases[0, pl.ds(span, 1), :]
            base_sin = bases[1, pl.ds(span, 1), :]
            cosines.append(base_cos * inners[0] - base_sin * inners[1])
            sines.append(base_sin * inners[2] + base_cos * inners[3])
            starts.append(span * span_len)
        return jnp.concatenate(cosines, 0), jnp.concatenate(sines, 0), starts

    def rotate(values, cosine, sine):
        values = values.astype(jnp.float32)
        turned = pltpu.roll(values, HEAD_DIM // 2, 1)
        return (values * cosine + turned * sine).astype(jnp.bfloat16)

    def positions(starts, shape, axis):
        index = lax.broadcasted_iota(jnp.int32, shape, axis)
        result = starts[0] + index
        for at in range(1, len(starts)):
            result = jnp.where(index < at * span_len, result, starts[at] + index - at * span_len)
        return result

    own_cos, own_sin, own_starts = angles(me)
    own_places = positions(own_starts, (rows, 1), 0)
    for head in range(kv_local * GROUP):
        q_rot[head // GROUP, pl.ds(head % GROUP * rows, rows), :] = rotate(
            q_in[:, head * HEAD_DIM:(head + 1) * HEAD_DIM], own_cos, own_sin)

    def dot_nt(a, b):
        return lax.dot_general(a, b, (((1,), (1,)), ((), ())), preferred_element_type=jnp.float32)

    def join(pieces):
        return pieces[0] if len(pieces) == 1 else jnp.concatenate(pieces, 0)

    def block(items, first=False, last=False):
        parts = [angles(flipped(me, item)) for item in items]
        cosine, sine = join([p[0] for p in parts]), join([p[1] for p in parts])
        width = rows * len(items)
        allowed = positions(sum([p[2] for p in parts], []), (1, width), 1) <= own_places
        for head in range(kv_local):
            columns = slice(head * HEAD_DIM, (head + 1) * HEAD_DIM)
            keys = rotate(join([text[item, 0, :, columns] for item in items]), cosine, sine)
            scores = dot_nt(q_rot[head], keys) * SCALE
            scores = jnp.where(allowed[None], scores.reshape(GROUP, rows, width), NEG_FILL)
            scores = scores.reshape(GROUP * rows, width)
            top = jnp.max(scores, -1, keepdims=True)
            if not first:
                old = peak[head]
                top = jnp.maximum(top, old)
            weights = jnp.exp2(scores - top)
            summed = jnp.sum(weights, -1, keepdims=True)
            product = jnp.dot(
                weights.astype(jnp.bfloat16), join([text[item, 1, :, columns] for item in items]),
                preferred_element_type=jnp.float32)
            if not first:
                factor = jnp.exp2(old - top)
                summed = summed + total[head] * factor
                product = product + mixed[head] * factor
            if last:
                store(out_v, head, product / summed)
            else:
                peak[head] = top
                total[head] = summed
                mixed[head] = product

    def store(target, head, result):
        result = result.astype(jnp.bfloat16)
        for g in range(GROUP):
            at = head * GROUP + g
            target[:, at * HEAD_DIM:(at + 1) * HEAD_DIM] = result[g * rows:(g + 1) * rows]

    def cross():
        keys_all = image[:, 0].astype(jnp.float32).reshape(n * image_rows, -1).astype(jnp.bfloat16)
        values_all = image[:, 1].astype(jnp.float32).reshape(n * image_rows, -1).astype(jnp.bfloat16)
        for head in range(kv_local):
            columns = slice(head * HEAD_DIM, (head + 1) * HEAD_DIM)
            queries = jnp.concatenate(
                [cq_in[:, h * HEAD_DIM:(h + 1) * HEAD_DIM] for h in range(head * GROUP, (head + 1) * GROUP)], 0)
            scores = dot_nt(queries, keys_all[:, columns]) * SCALE
            weights = jnp.exp2(scores - jnp.max(scores, -1, keepdims=True))
            summed = jnp.sum(weights, -1, keepdims=True)
            product = jnp.dot(
                weights.astype(jnp.bfloat16), values_all[:, columns], preferred_element_type=jnp.float32)
            store(cout_v, head, product / summed)

    block([0], first=True)
    if n == 8 and nx == 2:
        arrive_text(4)
        arrive_text(2)
        arrive_image(4)
        arrive_text(1)
        arrive_image(1)
        arrive_image(5)
        block([1, 2, 4])
        arrive_text(6)
        for item in (2, 3, 6, 7):
            arrive_image(item)
        arrive_text(5)
        arrive_text(3)
        block([3, 5, 6])
        cross()
        arrive_text(7)
        block([7], last=True)
    else:
        for mask, held in text_steps:
            for item in held:
                arrive_text(item ^ mask)
        for mask, held in image_steps:
            for item in held:
                arrive_image(item ^ mask)

        def step(item, unused):
            block([item])
            return 0

        lax.fori_loop(1, n, step, 0)
        for head in range(kv_local):
            store(out_v, head, mixed[head] / total[head])
        cross()
    for copy in started:
        copy.wait_send()


def body(n, nx, self_queries, self_keys, self_values, cross_queries, cross_keys, cross_values, span_order):
    rows, width = self_queries.shape
    kv_width = self_keys.shape[1]
    kv_local = kv_width // HEAD_DIM
    image_rows = cross_keys.shape[0]
    bases, inners = rotary_tables(span_order.shape[0], rows // 2)
    anywhere = pl.BlockSpec(memory_space=pl.ANY)
    ways = n.bit_length() - 1
    result = pltpu.VMEM((rows, width), jnp.bfloat16)
    return pl.pallas_call(
        functools.partial(kernel, n, nx),
        out_shape=(result, result),
        in_specs=[pl.BlockSpec(memory_space=pltpu.SMEM)] + [anywhere] * 8,
        out_specs=(pl.BlockSpec(memory_space=pltpu.VMEM),) * 2,
        scratch_shapes=[
            pltpu.VMEM((n, 2, rows, kv_width), jnp.bfloat16),
            pltpu.VMEM((n, 2, image_rows, kv_width), jnp.bfloat16),
            pltpu.VMEM((rows, width), jnp.bfloat16),
            pltpu.VMEM((rows, width), jnp.bfloat16),
            pltpu.VMEM(bases.shape, jnp.float32),
            pltpu.VMEM(inners.shape, jnp.float32),
            pltpu.VMEM((kv_local, GROUP * rows, HEAD_DIM), jnp.bfloat16),
            pltpu.VMEM((kv_local, GROUP * rows, 1), jnp.float32),
            pltpu.VMEM((kv_local, GROUP * rows, 1), jnp.float32),
            pltpu.VMEM((kv_local, GROUP * rows, HEAD_DIM), jnp.float32),
            pltpu.SemaphoreType.DMA((8,)),
            pltpu.SemaphoreType.DMA((n, 2, ways)),
            pltpu.SemaphoreType.DMA((n, 2)),
            pltpu.SemaphoreType.DMA((n, ways)),
            pltpu.SemaphoreType.DMA((n,)),
        ],
        compiler_params=pltpu.CompilerParams(collective_id=0, has_side_effects=True),
    )(span_order, self_queries, self_keys, self_values, cross_queries, cross_keys, cross_values, bases, inners)


def fast_axis(mesh, n):
    line = mesh.devices[0, :, 0]
    coords = [getattr(device, "coords", None) for device in line]
    if any(c is None for c in coords):
        return 1
    nx = len({c[0] for c in coords})
    return nx if n % nx == 0 else 1


def solution(mesh):
    n = mesh.shape["context"]
    both = P(("groups", "context"), "tensor")
    return jax.shard_map(
        functools.partial(body, n, fast_axis(mesh, n)), mesh=mesh,
        in_specs=(both,) * 6 + (P("groups"),), out_specs=(both, both), check_vma=False)
```

```python
import functools
import math

import jax
import jax.numpy as jnp
import numpy as np
from jax import lax
from jax.experimental import pallas as pl
from jax.experimental.pallas import tpu as pltpu
from jax.sharding import PartitionSpec as P

HEAD_DIM = 128
HEADS = 16
KV_HEADS = 4
GROUP = HEADS // KV_HEADS
NEG_FILL = -1e30
SCALE = HEAD_DIM ** (-0.5) * math.log2(math.e)


def rotary_tables(spans, span_len):
    half = HEAD_DIM // 2
    frequency = 500000.0 ** (-(np.arange(half) * 2.0) / HEAD_DIM)
    frequency = np.concatenate([frequency, frequency])
    base = (np.arange(spans) * span_len)[:, None] * frequency[None, :]
    inner = np.arange(span_len)[:, None] * frequency[None, :]
    sign = np.where(np.arange(HEAD_DIM) < half, -1.0, 1.0)[None, :]
    bases = np.stack([np.cos(base), np.sin(base)])
    inners = np.stack([np.cos(inner), np.sin(inner), np.cos(inner) * sign, np.sin(inner) * sign])
    return bases.astype(np.float32), inners.astype(np.float32)


def doubling(order):
    held, steps = [0], []
    for mask in order:
        steps.append((mask, list(held)))
        held += [item ^ mask for item in held]
    return steps


def kernel(
    n, nx,
    order, q_hbm, k_hbm, v_hbm, cq_hbm, ck_hbm, cv_hbm, bases_hbm, inners_hbm,
    out_v, cout_v,
    text, image, q_in, cq_in, bases, inners, q_rot, peak, total, mixed,
    load_sem, text_send, text_recv, image_send, image_recv,
):
    me = lax.axis_index("context")
    rows = q_in.shape[0]
    span_len = rows // 2
    kv_local = text.shape[3] // HEAD_DIM
    image_rows = image.shape[2]

    x_masks = [1 << b for b in reversed(range(nx.bit_length() - 1))]
    z_masks = [nx << b for b in reversed(range((n // nx).bit_length() - 1))]
    masks = z_masks + x_masks
    z_x = doubling(z_masks + x_masks)
    z_x_z = doubling(z_masks[:1] + x_masks + z_masks[1:])
    x_z = doubling(x_masks + z_masks)
    part_steps = (z_x, z_x)
    image_steps = x_z

    def flipped(index, item):
        for mask in masks:
            bit = (item // mask) % 2
            index = index + mask * bit * (1 - 2 * ((index // mask) % 2))
        return index

    partner = {mask: flipped(me, mask) for mask in masks}

    barrier = pltpu.get_barrier_semaphore()
    for mask in masks:
        pl.semaphore_signal(
            barrier, inc=1, device_id={"context": partner[mask]},
            device_id_type=pl.DeviceIdType.MESH)
    kv_loads = [
        pltpu.make_async_copy(k_hbm, text.at[0, 0], load_sem.at[0]),
        pltpu.make_async_copy(v_hbm, text.at[0, 1], load_sem.at[1]),
        pltpu.make_async_copy(ck_hbm, image.at[0, 0], load_sem.at[2]),
        pltpu.make_async_copy(cv_hbm, image.at[0, 1], load_sem.at[3]),
    ]
    other_loads = [
        pltpu.make_async_copy(bases_hbm, bases, load_sem.at[4]),
        pltpu.make_async_copy(inners_hbm, inners, load_sem.at[5]),
        pltpu.make_async_copy(q_hbm, q_in, load_sem.at[6]),
        pltpu.make_async_copy(cq_hbm, cq_in, load_sem.at[7]),
    ]
    for load in kv_loads:
        load.start()
    for load in other_loads:
        load.start()
    for load in kv_loads:
        load.wait()
    pl.semaphore_wait(barrier, len(masks))

    started = []

    def text_copy(item, part, mask):
        way = masks.index(mask)
        return pltpu.make_async_remote_copy(
            src_ref=text.at[item, part], dst_ref=text.at[item ^ mask, part],
            send_sem=text_send.at[item, part, way], recv_sem=text_recv.at[item ^ mask, part],
            device_id={"context": partner[mask]}, device_id_type=pl.DeviceIdType.MESH)

    def image_copy(item, mask):
        way = masks.index(mask)
        return pltpu.make_async_remote_copy(
            src_ref=image.at[item], dst_ref=image.at[item ^ mask],
            send_sem=image_send.at[item, way], recv_sem=image_recv.at[item ^ mask],
            device_id={"context": partner[mask]}, device_id_type=pl.DeviceIdType.MESH)

    def start(copy):
        copy.start()
        started.append(copy)

    def forward_text(item, part):
        for mask, held in part_steps[part]:
            if item in held:
                start(text_copy(item, part, mask))

    def forward_image(item):
        for mask, held in image_steps:
            if item in held:
                start(image_copy(item, mask))

    def arrive_text(item, part):
        text_copy(item ^ masks[0], part, masks[0]).wait_recv()
        forward_text(item, part)

    def arrive_image(item):
        image_copy(item ^ masks[0], masks[0]).wait_recv()
        forward_image(item)

    forward_text(0, 0)
    forward_text(0, 1)
    forward_image(0)

    for load in other_loads:
        load.wait()

    def angles(place):
        cosines, sines, starts = [], [], []
        for part in range(2):
            span = order[2 * place + part]
            base_cos = bases[0, pl.ds(span, 1), :]
            base_sin = bases[1, pl.ds(span, 1), :]
            cosines.append(base_cos * inners[0] - base_sin * inners[1])
            sines.append(base_sin * inners[2] + base_cos * inners[3])
            starts.append(span * span_len)
        return jnp.concatenate(cosines, 0), jnp.concatenate(sines, 0), starts

    def rotate(values, cosine, sine):
        values = values.astype(jnp.float32)
        turned = pltpu.roll(values, HEAD_DIM // 2, 1)
        return (values * cosine + turned * sine).astype(jnp.bfloat16)

    def positions(starts, shape, axis):
        index = lax.broadcasted_iota(jnp.int32, shape, axis)
        result = starts[0] + index
        for at in range(1, len(starts)):
            result = jnp.where(index < at * span_len, result, starts[at] + index - at * span_len)
        return result

    own_cos, own_sin, own_starts = angles(me)
    own_places = positions(own_starts, (rows, 1), 0)
    for head in range(kv_local * GROUP):
        q_rot[head // GROUP, pl.ds(head % GROUP * rows, rows), :] = rotate(
            q_in[:, head * HEAD_DIM:(head + 1) * HEAD_DIM], own_cos, own_sin)

    def dot_nt(a, b):
        return lax.dot_general(a, b, (((1,), (1,)), ((), ())), preferred_element_type=jnp.float32)

    def join(pieces):
        return pieces[0] if len(pieces) == 1 else jnp.concatenate(pieces, 0)

    def block(items, first=False, last=False):
        parts = [angles(flipped(me, item)) for item in items]
        cosine, sine = join([p[0] for p in parts]), join([p[1] for p in parts])
        width = rows * len(items)
        allowed = positions(sum([p[2] for p in parts], []), (1, width), 1) <= own_places
        for head in range(kv_local):
            columns = slice(head * HEAD_DIM, (head + 1) * HEAD_DIM)
            keys = rotate(join([text[item, 0, :, columns] for item in items]), cosine, sine)
            scores = dot_nt(q_rot[head], keys) * SCALE
            scores = jnp.where(allowed[None], scores.reshape(GROUP, rows, width), NEG_FILL)
            scores = scores.reshape(GROUP * rows, width)
            top = jnp.max(scores, -1, keepdims=True)
            if not first:
                old = peak[head]
                top = jnp.maximum(top, old)
            weights = jnp.exp2(scores - top)
            summed = jnp.sum(weights, -1, keepdims=True)
            product = jnp.dot(
                weights.astype(jnp.bfloat16), join([text[item, 1, :, columns] for item in items]),
                preferred_element_type=jnp.float32)
            if not first:
                factor = jnp.exp2(old - top)
                summed = summed + total[head] * factor
                product = product + mixed[head] * factor
            if last:
                store(out_v, head, product / summed)
            else:
                peak[head] = top
                total[head] = summed
                mixed[head] = product

    def store(target, head, result):
        result = result.astype(jnp.bfloat16)
        for g in range(GROUP):
            at = head * GROUP + g
            target[:, at * HEAD_DIM:(at + 1) * HEAD_DIM] = result[g * rows:(g + 1) * rows]

    def cross():
        keys_all = image[:, 0].astype(jnp.float32).reshape(n * image_rows, -1).astype(jnp.bfloat16)
        values_all = image[:, 1].astype(jnp.float32).reshape(n * image_rows, -1).astype(jnp.bfloat16)
        for head in range(kv_local):
            columns = slice(head * HEAD_DIM, (head + 1) * HEAD_DIM)
            queries = jnp.concatenate(
                [cq_in[:, h * HEAD_DIM:(h + 1) * HEAD_DIM] for h in range(head * GROUP, (head + 1) * GROUP)], 0)
            scores = dot_nt(queries, keys_all[:, columns]) * SCALE
            weights = jnp.exp2(scores - jnp.max(scores, -1, keepdims=True))
            summed = jnp.sum(weights, -1, keepdims=True)
            product = jnp.dot(
                weights.astype(jnp.bfloat16), values_all[:, columns], preferred_element_type=jnp.float32)
            store(cout_v, head, product / summed)

    def run_events(events):
        for event in events.split():
            kind, items = event[0], [int(digit) for digit in event[1:]]
            if kind == "B":
                block(items)
            elif kind == "L":
                block(items, last=True)
            elif kind == "C":
                cross()
            elif kind == "i":
                for item in items:
                    arrive_image(item)
            else:
                for item in items:
                    arrive_text(item, "KV".index(kind))

    block([0], first=True)
    if n == 8 and nx == 2:
        run_events(
            'K4 V4 K2 V2 K1 V1 i1 i4 B124 K6 V6 i5 K3 V3 K5 V5 B356 i2367 C K7 V7 L7')
    else:
        for part in range(2):
            for mask, held in part_steps[part]:
                for item in held:
                    arrive_text(item ^ mask, part)
        for mask, held in image_steps:
            for item in held:
                arrive_image(item ^ mask)

        def step(item, unused):
            block([item])
            return 0

        lax.fori_loop(1, n, step, 0)
        for head in range(kv_local):
            store(out_v, head, mixed[head] / total[head])
        cross()
    for copy in started:
        copy.wait_send()


def flush(self_v, cross_v, self_hbm, cross_hbm, sems):
    copies = [
        pltpu.make_async_copy(self_v, self_hbm, sems.at[0]),
        pltpu.make_async_copy(cross_v, cross_hbm, sems.at[1]),
    ]
    for copy in copies:
        copy.start()
    for copy in copies:
        copy.wait()


def body(n, nx, self_queries, self_keys, self_values, cross_queries, cross_keys, cross_values, span_order):
    rows, width = self_queries.shape
    kv_width = self_keys.shape[1]
    kv_local = kv_width // HEAD_DIM
    image_rows = cross_keys.shape[0]
    bases, inners = rotary_tables(span_order.shape[0], rows // 2)
    anywhere = pl.BlockSpec(memory_space=pl.ANY)
    ways = n.bit_length() - 1
    result = pltpu.VMEM((rows, width), jnp.bfloat16)
    held = pl.pallas_call(
        functools.partial(kernel, n, nx),
        out_shape=(result, result),
        in_specs=[pl.BlockSpec(memory_space=pltpu.SMEM)] + [anywhere] * 8,
        out_specs=(pl.BlockSpec(memory_space=pltpu.VMEM),) * 2,
        scratch_shapes=[
            pltpu.VMEM((n, 2, rows, kv_width), jnp.bfloat16),
            pltpu.VMEM((n, 2, image_rows, kv_width), jnp.bfloat16),
            pltpu.VMEM((rows, width), jnp.bfloat16),
            pltpu.VMEM((rows, width), jnp.bfloat16),
            pltpu.VMEM(bases.shape, jnp.float32),
            pltpu.VMEM(inners.shape, jnp.float32),
            pltpu.VMEM((kv_local, GROUP * rows, HEAD_DIM), jnp.bfloat16),
            pltpu.VMEM((kv_local, GROUP * rows, 1), jnp.float32),
            pltpu.VMEM((kv_local, GROUP * rows, 1), jnp.float32),
            pltpu.VMEM((kv_local, GROUP * rows, HEAD_DIM), jnp.float32),
            pltpu.SemaphoreType.DMA((8,)),
            pltpu.SemaphoreType.DMA((n, 2, ways)),
            pltpu.SemaphoreType.DMA((n, 2)),
            pltpu.SemaphoreType.DMA((n, ways)),
            pltpu.SemaphoreType.DMA((n,)),
        ],
        compiler_params=pltpu.CompilerParams(collective_id=0, has_side_effects=True),
    )(span_order, self_queries, self_keys, self_values, cross_queries, cross_keys, cross_values, bases, inners)
    plain = jax.ShapeDtypeStruct((rows, width), jnp.bfloat16)
    return pl.pallas_call(
        flush,
        out_shape=(plain, plain),
        in_specs=[pl.BlockSpec(memory_space=pltpu.VMEM)] * 2,
        out_specs=(anywhere, anywhere),
        scratch_shapes=[pltpu.SemaphoreType.DMA((2,))],
    )(*[pltpu.with_memory_space_constraint(array, pltpu.VMEM) for array in held])


def fast_axis(mesh, n):
    line = mesh.devices[0, :, 0]
    coords = [getattr(device, "coords", None) for device in line]
    if any(c is None for c in coords):
        return 1
    nx = len({c[0] for c in coords})
    return nx if n % nx == 0 else 1


def solution(mesh):
    n = mesh.shape["context"]
    both = P(("groups", "context"), "tensor")
    return jax.shard_map(
        functools.partial(body, n, fast_axis(mesh, n)), mesh=mesh,
        in_specs=(both,) * 6 + (P("groups"),), out_specs=(both, both), check_vma=False)
```

```python
import functools
import math

import jax
import jax.numpy as jnp
import numpy as np
from jax import lax
from jax.experimental import pallas as pl
from jax.experimental.pallas import tpu as pltpu
from jax.sharding import PartitionSpec as P

HEAD_DIM = 128
HEADS = 16
KV_HEADS = 4
GROUP = HEADS // KV_HEADS
NEG_FILL = -1e30
SCALE = HEAD_DIM ** (-0.5) * math.log2(math.e)


def rotary_tables(spans, span_len):
    half = HEAD_DIM // 2
    frequency = 500000.0 ** (-(np.arange(half) * 2.0) / HEAD_DIM)
    frequency = np.concatenate([frequency, frequency])
    base = (np.arange(spans) * span_len)[:, None] * frequency[None, :]
    inner = np.arange(span_len)[:, None] * frequency[None, :]
    sign = np.where(np.arange(HEAD_DIM) < half, -1.0, 1.0)[None, :]
    bases = np.stack([np.cos(base), np.sin(base)])
    inners = np.stack([np.cos(inner), np.sin(inner), np.cos(inner) * sign, np.sin(inner) * sign])
    return bases.astype(np.float32), inners.astype(np.float32)


def doubling(order):
    held, steps = [0], []
    for mask in order:
        steps.append((mask, list(held)))
        held += [item ^ mask for item in held]
    return steps


def kernel(
    n, nx,
    order, q_hbm, k_hbm, v_hbm, cq_hbm, ck_hbm, cv_hbm, bases_hbm, inners_hbm,
    out_v, cout_v,
    text, image, q_in, cq_in, bases, inners, q_rot, peak, total, mixed,
    load_sem, text_send, text_recv, image_send, image_recv,
):
    me = lax.axis_index("context")
    rows = q_in.shape[0]
    span_len = rows // 2
    kv_local = text.shape[3] // HEAD_DIM
    image_rows = image.shape[2]

    x_masks = [1 << b for b in reversed(range(nx.bit_length() - 1))]
    z_masks = [nx << b for b in reversed(range((n // nx).bit_length() - 1))]
    masks = z_masks + x_masks
    z_x = doubling(z_masks + x_masks)
    z_x_z = doubling(z_masks[:1] + x_masks + z_masks[1:])
    x_z = doubling(x_masks + z_masks)
    part_steps = (z_x, z_x)
    image_steps = x_z

    def flipped(index, item):
        for mask in masks:
            bit = (item // mask) % 2
            index = index + mask * bit * (1 - 2 * ((index // mask) % 2))
        return index

    partner = {mask: flipped(me, mask) for mask in masks}

    barrier = pltpu.get_barrier_semaphore()
    for mask in masks:
        pl.semaphore_signal(
            barrier, inc=1, device_id={"context": partner[mask]},
            device_id_type=pl.DeviceIdType.MESH)
    kv_loads = [
        pltpu.make_async_copy(k_hbm, text.at[0, 0], load_sem.at[0]),
        pltpu.make_async_copy(v_hbm, text.at[0, 1], load_sem.at[1]),
        pltpu.make_async_copy(ck_hbm, image.at[0, 0], load_sem.at[2]),
        pltpu.make_async_copy(cv_hbm, image.at[0, 1], load_sem.at[3]),
    ]
    other_loads = [
        pltpu.make_async_copy(bases_hbm, bases, load_sem.at[4]),
        pltpu.make_async_copy(inners_hbm, inners, load_sem.at[5]),
        pltpu.make_async_copy(q_hbm, q_in, load_sem.at[6]),
        pltpu.make_async_copy(cq_hbm, cq_in, load_sem.at[7]),
    ]
    for load in kv_loads:
        load.start()
    for load in other_loads:
        load.start()
    for load in kv_loads:
        load.wait()
    pl.semaphore_wait(barrier, len(masks))

    started = []

    def text_copy(item, part, mask):
        way = masks.index(mask)
        return pltpu.make_async_remote_copy(
            src_ref=text.at[item, part], dst_ref=text.at[item ^ mask, part],
            send_sem=text_send.at[item, part, way], recv_sem=text_recv.at[item ^ mask, part],
            device_id={"context": partner[mask]}, device_id_type=pl.DeviceIdType.MESH)

    def image_copy(item, mask):
        way = masks.index(mask)
        return pltpu.make_async_remote_copy(
            src_ref=image.at[item], dst_ref=image.at[item ^ mask],
            send_sem=image_send.at[item, way], recv_sem=image_recv.at[item ^ mask],
            device_id={"context": partner[mask]}, device_id_type=pl.DeviceIdType.MESH)

    def start(copy):
        copy.start()
        started.append(copy)

    def forward_text(item, part):
        for mask, held in part_steps[part]:
            if item in held:
                start(text_copy(item, part, mask))

    def forward_image(item):
        for mask, held in image_steps:
            if item in held:
                start(image_copy(item, mask))

    def arrive_text(item, part):
        text_copy(item ^ masks[0], part, masks[0]).wait_recv()
        forward_text(item, part)

    def arrive_image(item):
        image_copy(item ^ masks[0], masks[0]).wait_recv()
        forward_image(item)

    forward_text(0, 0)
    forward_text(0, 1)
    forward_image(0)

    for load in other_loads:
        load.wait()

    def angles(place):
        cosines, sines, starts = [], [], []
        for part in range(2):
            span = order[2 * place + part]
            base_cos = bases[0, pl.ds(span, 1), :]
            base_sin = bases[1, pl.ds(span, 1), :]
            cosines.append(base_cos * inners[0] - base_sin * inners[1])
            sines.append(base_sin * inners[2] + base_cos * inners[3])
            starts.append(span * span_len)
        return jnp.concatenate(cosines, 0), jnp.concatenate(sines, 0), starts

    def rotate(values, cosine, sine):
        values = values.astype(jnp.float32)
        turned = pltpu.roll(values, HEAD_DIM // 2, 1)
        return (values * cosine + turned * sine).astype(jnp.bfloat16)

    def positions(starts, shape, axis):
        index = lax.broadcasted_iota(jnp.int32, shape, axis)
        result = starts[0] + index
        for at in range(1, len(starts)):
            result = jnp.where(index < at * span_len, result, starts[at] + index - at * span_len)
        return result

    own_cos, own_sin, own_starts = angles(me)
    own_places = positions(own_starts, (rows, 1), 0)
    for head in range(kv_local * GROUP):
        q_rot[head // GROUP, pl.ds(head % GROUP * rows, rows), :] = rotate(
            q_in[:, head * HEAD_DIM:(head + 1) * HEAD_DIM], own_cos, own_sin)

    def dot_nt(a, b):
        return lax.dot_general(a, b, (((1,), (1,)), ((), ())), preferred_element_type=jnp.float32)

    def join(pieces):
        return pieces[0] if len(pieces) == 1 else jnp.concatenate(pieces, 0)

    def block(items, first=False, last=False):
        parts = [angles(flipped(me, item)) for item in items]
        cosine, sine = join([p[0] for p in parts]), join([p[1] for p in parts])
        width = rows * len(items)
        allowed = positions(sum([p[2] for p in parts], []), (1, width), 1) <= own_places
        for head in range(kv_local):
            columns = slice(head * HEAD_DIM, (head + 1) * HEAD_DIM)
            keys = rotate(join([text[item, 0, :, columns] for item in items]), cosine, sine)
            scores = dot_nt(q_rot[head], keys) * SCALE
            scores = jnp.where(allowed[None], scores.reshape(GROUP, rows, width), NEG_FILL)
            scores = scores.reshape(GROUP * rows, width)
            top = jnp.max(scores, -1, keepdims=True)
            if not first:
                old = peak[head]
                top = jnp.maximum(top, old)
            weights = jnp.exp2(scores - top)
            summed = jnp.sum(weights, -1, keepdims=True)
            product = jnp.dot(
                weights.astype(jnp.bfloat16), join([text[item, 1, :, columns] for item in items]),
                preferred_element_type=jnp.float32)
            if not first:
                factor = jnp.exp2(old - top)
                summed = summed + total[head] * factor
                product = product + mixed[head] * factor
            if last:
                store(out_v, head, product / summed)
            else:
                peak[head] = top
                total[head] = summed
                mixed[head] = product

    def store(target, head, result):
        result = result.astype(jnp.bfloat16)
        for g in range(GROUP):
            at = head * GROUP + g
            target[:, at * HEAD_DIM:(at + 1) * HEAD_DIM] = result[g * rows:(g + 1) * rows]

    def cross():
        keys_all = image[:, 0].astype(jnp.float32).reshape(n * image_rows, -1).astype(jnp.bfloat16)
        values_all = image[:, 1].astype(jnp.float32).reshape(n * image_rows, -1).astype(jnp.bfloat16)
        for head in range(kv_local):
            columns = slice(head * HEAD_DIM, (head + 1) * HEAD_DIM)
            queries = jnp.concatenate(
                [cq_in[:, h * HEAD_DIM:(h + 1) * HEAD_DIM] for h in range(head * GROUP, (head + 1) * GROUP)], 0)
            scores = dot_nt(queries, keys_all[:, columns]) * SCALE
            weights = jnp.exp2(scores - jnp.max(scores, -1, keepdims=True))
            summed = jnp.sum(weights, -1, keepdims=True)
            product = jnp.dot(
                weights.astype(jnp.bfloat16), values_all[:, columns], preferred_element_type=jnp.float32)
            store(cout_v, head, product / summed)

    def run_events(events):
        for event in events:
            kind, items = event[0], [int(digit) for digit in event[1:]]
            if kind == "B":
                block(items)
            elif kind == "L":
                block(items, last=True)
            elif kind == "C":
                cross()
            elif kind == "i":
                for item in items:
                    arrive_image(item)
            else:
                for item in items:
                    arrive_text(item, "KV".index(kind))

    block([0], first=True)
    if n == 8 and nx == 2:
        run_events((
            "K4", "V4", "K2", "V2", "K1", "V1", "i1", "i4", "B124", "K6", "V6", "i5",
            "K3", "V3", "K5", "V5", "B356", "i2367", "C", "K7", "V7", "L7"))
    else:
        for part in range(2):
            for mask, held in part_steps[part]:
                for item in held:
                    arrive_text(item ^ mask, part)
        for mask, held in image_steps:
            for item in held:
                arrive_image(item ^ mask)

        def step(item, unused):
            block([item])
            return 0

        lax.fori_loop(1, n, step, 0)
        for head in range(kv_local):
            store(out_v, head, mixed[head] / total[head])
        cross()
    for copy in started:
        copy.wait_send()


def flush(self_v, cross_v, self_hbm, cross_hbm, sems):
    copies = [
        pltpu.make_async_copy(self_v, self_hbm, sems.at[0]),
        pltpu.make_async_copy(cross_v, cross_hbm, sems.at[1]),
    ]
    for copy in copies:
        copy.start()
    for copy in copies:
        copy.wait()


def body(n, nx, self_queries, self_keys, self_values, cross_queries, cross_keys, cross_values, span_order):
    rows, width = self_queries.shape
    kv_width = self_keys.shape[1]
    kv_local = kv_width // HEAD_DIM
    image_rows = cross_keys.shape[0]
    bases, inners = rotary_tables(span_order.shape[0], rows // 2)
    anywhere = pl.BlockSpec(memory_space=pl.ANY)
    ways = n.bit_length() - 1
    result = pltpu.VMEM((rows, width), jnp.bfloat16)
    held = pl.pallas_call(
        functools.partial(kernel, n, nx),
        out_shape=(result, result),
        in_specs=[pl.BlockSpec(memory_space=pltpu.SMEM)] + [anywhere] * 8,
        out_specs=(pl.BlockSpec(memory_space=pltpu.VMEM),) * 2,
        scratch_shapes=[
            pltpu.VMEM((n, 2, rows, kv_width), jnp.bfloat16),
            pltpu.VMEM((n, 2, image_rows, kv_width), jnp.bfloat16),
            pltpu.VMEM((rows, width), jnp.bfloat16),
            pltpu.VMEM((rows, width), jnp.bfloat16),
            pltpu.VMEM(bases.shape, jnp.float32),
            pltpu.VMEM(inners.shape, jnp.float32),
            pltpu.VMEM((kv_local, GROUP * rows, HEAD_DIM), jnp.bfloat16),
            pltpu.VMEM((kv_local, GROUP * rows, 1), jnp.float32),
            pltpu.VMEM((kv_local, GROUP * rows, 1), jnp.float32),
            pltpu.VMEM((kv_local, GROUP * rows, HEAD_DIM), jnp.float32),
            pltpu.SemaphoreType.DMA((8,)),
            pltpu.SemaphoreType.DMA((n, 2, ways)),
            pltpu.SemaphoreType.DMA((n, 2)),
            pltpu.SemaphoreType.DMA((n, ways)),
            pltpu.SemaphoreType.DMA((n,)),
        ],
        compiler_params=pltpu.CompilerParams(collective_id=0, has_side_effects=True),
    )(span_order, self_queries, self_keys, self_values, cross_queries, cross_keys, cross_values, bases, inners)
    plain = jax.ShapeDtypeStruct((rows, width), jnp.bfloat16)
    return pl.pallas_call(
        flush,
        out_shape=(plain, plain),
        in_specs=[pl.BlockSpec(memory_space=pltpu.VMEM)] * 2,
        out_specs=(anywhere, anywhere),
        scratch_shapes=[pltpu.SemaphoreType.DMA((2,))],
    )(*[pltpu.with_memory_space_constraint(array, pltpu.VMEM) for array in held])


def fast_axis(mesh, n):
    line = mesh.devices[0, :, 0]
    coords = [getattr(device, "coords", None) for device in line]
    if any(c is None for c in coords):
        return 1
    nx = len({c[0] for c in coords})
    return nx if n % nx == 0 else 1


def solution(mesh):
    n = mesh.shape["context"]
    both = P(("groups", "context"), "tensor")
    return jax.shard_map(
        functools.partial(body, n, fast_axis(mesh, n)), mesh=mesh,
        in_specs=(both,) * 6 + (P("groups"),), out_specs=(both, both), check_vma=False)
```
